512 devices in a mesh: sec: 32 (over x, y), day: 16 (over z, core).
Axes of the slice: x: 4, y: 8, z: 8, core: 2. Of those that a mesh axis runs over, the one named last changes fastest.
Arguments:
- sec_pnl: bfloat16 [32768, 2048], P('sec', 'day'), may hold values from -6 to 6
- holdings: bfloat16 [512, 128, 128], P('sec'), may hold values from -0.0546875 to 0.0546875
- tile_pblock: int32 [512], P('sec'), may hold values from 0 to 1, as said below
- tile_sblock: int32 [512], P('sec'), may hold values from 0 to 7
- tile_count: int32 [32], P('sec'), may hold values from 4 to 16, as said below
- tail_days: int32 [256, 103], replicated, may hold values from 0 to 2047, as said below
Outputs:
- pnl: bfloat16 [256, 2048], P('sec', 'day')
- shortfall: float32 [256], P('sec')
- tail_mean: float32 [512, 128, 128], P(('sec', 'day'))
The draws below stay inside these ranges and needn't reach their ends.
Inputs may be any that keep to these rules, and one draw needn't show every extreme that they name: On each security device the pairs (tile_pblock, tile_sblock) of its 16 slots are distinct. `tile_count`: some security device has all 16 slots live in every draw. `tail_days`: each row holds 103 distinct days.
All inputs are finite; a program needn't handle non-finite values.
Results may differ from the reference program's by a relative error of at most 0.0015.
Values may be sent and summed in bfloat16 or wider, within the bound.
No kernel may reach another device: no remote copies, remote signals or barrier semaphores. Data moves between devices by JAX's collectives and lax.ppermute only.
A program may use at most 64 MiB of HBM per device.

```python
import jax
import jax.numpy as jnp
from jax import lax

SB = 128
PB = 128
DAYS = 2048
TAIL = 103
SBLK_DEV = 8
PBLK = 2
CAP = 16
TILES = 512
SECS = 32768
N_SEC = 32


def tile_pairs(key):
    keys = jax.random.split(jax.random.fold_in(key, 7), N_SEC)

    def one_device(sub):
        order = jax.random.permutation(sub, PBLK * SBLK_DEV)[:CAP]
        return order.astype(jnp.int32)
    pairs = jax.vmap(one_device)(keys).reshape(-1)
    return (pairs // SBLK_DEV, pairs % SBLK_DEV)


def draw_tile_pblock(key, part):
    return tile_pairs(key)[0].astype(jnp.int32)


def draw_tile_sblock(key, part):
    return tile_pairs(key)[1].astype(jnp.int32)


def draw_tile_count(key, part):
    first, second = jax.random.split(jax.random.fold_in(key, 11))
    counts = jax.random.randint(first, (N_SEC,), CAP // 4, CAP // 2 + 1, dtype=jnp.int32)
    busiest = jax.random.randint(second, (), 0, N_SEC, dtype=jnp.int32)
    places = jnp.arange(N_SEC, dtype=jnp.int32)
    return jnp.where(places == busiest, CAP, counts).astype(jnp.int32)


def draw_tail_days(key, part):
    keys = jax.random.split(jax.random.fold_in(key, 13), PBLK * PB)

    def one_row(sub):
        return jax.random.permutation(sub, DAYS)[:TAIL].astype(jnp.int32)
    return jax.vmap(one_row)(keys)


def levels(own_key, dims, shards, low, largest):
    def one(axis_at, blocks):
        draws = jax.random.uniform(jax.random.fold_in(jax.random.fold_in(own_key, 6), axis_at), (blocks,), jnp.float32, low / len(shards), largest / len(shards))
        return jnp.repeat(jnp.exp(draws), dims[axis_at] // blocks).reshape((-1,) + (1,) * (len(dims) - axis_at - 1))

    factor_of = one(*shards[0])
    for cut in shards[1:]:
        factor_of = factor_of * one(*cut)
    return factor_of


def centred(stream_key, extent, spread, bound, cuts=(), held_as=jnp.bfloat16):
    level = levels(stream_key, extent, cuts, -0.22, 0.18) if cuts else 1.0
    array = jax.random.normal(stream_key, extent, jnp.float32) * spread * level
    return jnp.minimum(jnp.maximum(array, -bound), bound).astype(held_as)


def setup_inputs(seed: int = 0) -> dict:
    streams_of = jax.random.split(jax.random.key(seed), 7)
    sec_pnl = centred(streams_of[0], (SECS, DAYS), 1.0, 6.0, ((0, 32), (1, 16)))
    holdings = centred(streams_of[1], (TILES, PB, SB), (CAP * N_SEC * SB // PBLK // 3) ** -0.5, 0.0546875, ((0, 32),))
    tile_pblock = draw_tile_pblock(jax.random.fold_in(streams_of[6], 71), 0)
    tile_sblock = draw_tile_sblock(jax.random.fold_in(streams_of[6], 71), 0)
    tile_count = draw_tile_count(jax.random.fold_in(streams_of[6], 71), 0)
    tail_days = draw_tail_days(jax.random.fold_in(streams_of[6], 71), 0)
    return {"sec_pnl": sec_pnl, "holdings": holdings, "tile_pblock": tile_pblock, "tile_sblock": tile_sblock, "tile_count": tile_count, "tail_days": tail_days}


def reference(sec_pnl, holdings, tile_pblock, tile_sblock, tile_count, tail_days):
    slots_all = holdings.shape[0]
    positions = jnp.arange(slots_all, dtype=jnp.int32)
    device_of = positions // CAP
    alive = ((positions % CAP) < tile_count[device_of]).astype(jnp.float32)
    global_block = (device_of * SBLK_DEV + tile_sblock).astype(jnp.int32)

    def step(total, item):
        tile, pblock, sblock, flag = item
        block = lax.dynamic_slice_in_dim(sec_pnl, (sblock * SB).astype(jnp.int32), SB, 0)
        piece = jnp.dot(tile, block, preferred_element_type=jnp.float32) * flag
        start = (pblock * PB).astype(jnp.int32)
        current = lax.dynamic_slice_in_dim(total, start, PB, 0)
        return lax.dynamic_update_slice_in_dim(total, current + piece, start, 0), None

    total, _ = lax.scan(step, jnp.zeros((PBLK * PB, DAYS), jnp.float32),
                        (holdings, tile_pblock, global_block, alive))
    pnl = total.astype(jnp.bfloat16)
    picked = jnp.take_along_axis(total, tail_days.astype(jnp.int32), axis=1)
    shortfall = -jnp.sum(picked, axis=1) / TAIL

    def one_tile(item):
        pblock, sblock, flag = item
        block = lax.dynamic_slice_in_dim(sec_pnl, (sblock * SB).astype(jnp.int32), SB, 0).astype(jnp.float32)
        chosen = lax.dynamic_slice_in_dim(tail_days, (pblock * PB).astype(jnp.int32), PB, 0)
        values = jnp.take(block, chosen.astype(jnp.int32), axis=1)
        return jnp.sum(values, axis=2).T * flag / TAIL

    tail_mean = lax.map(one_tile, (tile_pblock, global_block, alive))
    return pnl, shortfall, tail_mean
```

```python
import functools

import jax
import jax.numpy as jnp
from jax import lax
from jax.experimental import pallas as pl
from jax.experimental.pallas import tpu as pltpu
from jax.sharding import PartitionSpec as P

SB = 128
PB = 128
TAIL = 103
LIMIT = 4 * 1024 * 1024
VMEM = pltpu.VMEM
SMEM = pltpu.SMEM


def spec(space):
    return pl.BlockSpec(memory_space=space)


def exchange(x, axis):
    return lax.all_to_all(x, axis, split_axis=0, concat_axis=0, tiled=True)


def partial_kernel(pb, sb, cnt, sec, hold, out, inv):
    slots = hold.shape[0]
    nsb = sec.shape[0] // SB
    npb = slots // nsb
    for t in range(slots):
        inv[pb[t] * nsb + sb[t]] = t
    for p in range(npb):
        acc = None
        for s in range(nsb):
            t = inv[p * nsb + s]
            live = (t < cnt[0]).astype(jnp.float32)
            term = live * jnp.dot(hold[t], sec[s * SB : (s + 1) * SB, :], preferred_element_type=jnp.float32)
            acc = term if acc is None else acc + term
        out[p * PB : (p + 1) * PB, :] = acc


def gather_kernel(sb, sec, out):
    for t in range(out.shape[0]):
        out[t] = sec[pl.ds(pl.multiple_of(sb[t] * SB, SB), SB), :]


def mask_kernel(pb, days, words, mine, turned):
    width = mine.shape[1]
    k = lax.axis_index("day")
    q = lax.axis_index("sec")
    nw = words.shape[0]
    first = k * width
    row = q * mine.shape[0]
    own = pl.ds(pl.multiple_of(pb[k] * PB, PB), PB)
    near = pl.ds(pl.multiple_of((row // PB) * PB, PB), PB)
    iw = lax.broadcasted_iota(jnp.int32, (nw, PB), 0)
    i8 = lax.broadcasted_iota(jnp.int32, (8, PB), 0)
    one = jnp.int32(1)
    acc = jnp.zeros((nw, PB), jnp.int32)
    loc = jnp.zeros((8, PB), jnp.int32)
    for j in range(0, TAIL, 8):
        n = min(8, TAIL - j)
        far = days[j : j + n, own]
        w = far & (nw - 1)
        b = lax.shift_left(jnp.full((n, PB), one), far // nw)
        here = days[j : j + n, near] - first
        inside = (here >= 0) & (here < width)
        hw = jnp.where(inside, here & 7, 8)
        hb = lax.shift_left(jnp.full((n, PB), one), jnp.where(inside, here // 8, 0))
        for r in range(n):
            acc = acc | jnp.where(iw == w[r : r + 1], b[r : r + 1], 0)
            loc = loc | jnp.where(i8 == hw[r : r + 1], hb[r : r + 1], 0)
    words[...] = acc
    local = jnp.concatenate([((loc >> b) & 1).astype(jnp.float32) for b in range(width // 8)], axis=0)
    turned[...] = local.T
    mine[...] = turned[pl.ds(pl.multiple_of(row % PB, 8), mine.shape[0]), :]


def share_kernel(arrived, mine, pnl, sums):
    share = jnp.sum(arrived[...], axis=0)
    pnl[...] = share.astype(jnp.bfloat16)
    picked = jnp.sum(share * mine[...], axis=1, keepdims=True)
    shape = share.shape
    diag = lax.broadcasted_iota(jnp.int32, shape, 0) == lax.broadcasted_iota(jnp.int32, shape, 1)
    line = jnp.sum(jnp.where(diag, picked, 0.0), axis=0, keepdims=True)
    for k in range(sums.shape[0]):
        sums[k] = line


def tail_kernel(cnt, words, blocks, out):
    bits = words[...]
    nw = bits.shape[0]
    per = SB // nw
    acc = None
    for k in range(blocks.shape[0]):
        mask = jnp.concatenate([((bits >> (k * per + i)) & 1).astype(jnp.float32) for i in range(per)], axis=0)
        term = jnp.dot(blocks[k], mask.astype(jnp.bfloat16), preferred_element_type=jnp.float32)
        acc = term if acc is None else acc + term
    live = (lax.axis_index("day") < cnt[0]).astype(jnp.float32)
    out[0] = acc.T * live / TAIL


def local(sec_pnl, holdings, tile_pblock, tile_sblock, tile_count, tail_days):
    n_day = lax.axis_size("day")
    n_sec = lax.axis_size("sec")
    width = sec_pnl.shape[1]
    slots = holdings.shape[0]
    portfolios = tail_days.shape[0]
    rows = portfolios // n_sec
    f32 = jnp.float32
    partial = pl.pallas_call(
        partial_kernel,
        out_shape=jax.ShapeDtypeStruct((portfolios, width), f32),
        in_specs=[spec(SMEM)] * 3 + [spec(VMEM)] * 2,
        out_specs=spec(VMEM),
        scratch_shapes=[pltpu.SMEM((slots,), jnp.int32)],
        cost_estimate=pl.CostEstimate(flops=2 * slots * SB * PB * width, bytes_accessed=900000, transcendentals=0),
        compiler_params=pltpu.CompilerParams(vmem_limit_bytes=LIMIT),
        name="partial",
    )(tile_pblock, tile_sblock, tile_count, sec_pnl, holdings)
    arrived = exchange(partial.reshape(n_sec, rows, width), "sec")
    selected = pl.pallas_call(
        gather_kernel,
        out_shape=jax.ShapeDtypeStruct((slots, SB, width), jnp.bfloat16),
        in_specs=[spec(SMEM), spec(VMEM)],
        out_specs=spec(VMEM),
        cost_estimate=pl.CostEstimate(flops=10**7, bytes_accessed=800000, transcendentals=0),
        compiler_params=pltpu.CompilerParams(vmem_limit_bytes=LIMIT),
        name="gather",
    )(tile_sblock, sec_pnl)
    blocks = exchange(selected, "day")
    words, mine = pl.pallas_call(
        mask_kernel,
        out_shape=(jax.ShapeDtypeStruct((n_day * width // 32, PB), jnp.int32), jax.ShapeDtypeStruct((rows, width), f32)),
        in_specs=[spec(SMEM), spec(VMEM)],
        out_specs=(spec(VMEM), spec(VMEM)),
        scratch_shapes=[pltpu.VMEM((PB, width), f32)],
        cost_estimate=pl.CostEstimate(flops=10**7, bytes_accessed=200000, transcendentals=0),
        compiler_params=pltpu.CompilerParams(vmem_limit_bytes=LIMIT),
        name="mask",
    )(tile_pblock, tail_days.T)
    pnl, sums = pl.pallas_call(
        share_kernel,
        out_shape=(jax.ShapeDtypeStruct((rows, width), jnp.bfloat16), jax.ShapeDtypeStruct((n_day, 1, 128), f32)),
        in_specs=[spec(VMEM)] * 2,
        out_specs=(spec(VMEM), spec(VMEM)),
        cost_estimate=pl.CostEstimate(flops=10**5, bytes_accessed=200000, transcendentals=0),
        compiler_params=pltpu.CompilerParams(vmem_limit_bytes=LIMIT),
        name="share",
    )(arrived, mine)
    total = exchange(sums, "day")
    shortfall = -(jnp.sum(total, axis=(0, 1))[:rows]) / TAIL
    tail_mean = pl.pallas_call(
        tail_kernel,
        out_shape=jax.ShapeDtypeStruct((1, PB, SB), f32),
        in_specs=[spec(SMEM)] + [spec(VMEM)] * 2,
        out_specs=spec(VMEM),
        cost_estimate=pl.CostEstimate(flops=2 * slots * SB * PB * width, bytes_accessed=700000, transcendentals=0),
        compiler_params=pltpu.CompilerParams(vmem_limit_bytes=LIMIT),
        name="tail",
    )(tile_count, words, blocks)
    return pnl, shortfall, tail_mean


def solution(mesh):
    placed = (P("sec", "day"), P("sec", None, None), P("sec"), P("sec"), P("sec"), P())
    return jax.shard_map(
        local,
        mesh=mesh,
        in_specs=placed,
        out_specs=(P("sec", "day"), P("sec"), P(("sec", "day"), None, None)),
        check_vma=False,
    )
```

```python
import jax
import jax.numpy as jnp
from jax import lax
from jax.experimental import pallas as pl
from jax.experimental.pallas import tpu as pltpu
from jax.sharding import PartitionSpec as P


SB = 128
PB = 128
TAIL = 103
LIMIT = 4 * 1024 * 1024
LOG2E = 1.4426950408889634
FULL = 32000.0
HIGH = 16000.0
VMEM = pltpu.VMEM
SMEM = pltpu.SMEM


def spec(space):
    return pl.BlockSpec(memory_space=space)


def exchange(x, axis):
    return lax.all_to_all(x, axis, split_axis=0, concat_axis=0, tiled=True)


def partial_kernel(pb, sb, cnt, sec, hold, out, inv):
    slots = hold.shape[0]
    nsb = sec.shape[0] // SB
    npb = slots // nsb
    for t in range(slots):
        inv[pb[t] * nsb + sb[t]] = t
    for p in range(npb):
        acc = None
        for s in range(nsb):
            t = inv[p * nsb + s]
            live = (t < cnt[0]).astype(jnp.float32)
            term = live * jnp.dot(hold[t], sec[s * SB : (s + 1) * SB, :], preferred_element_type=jnp.float32)
            acc = term if acc is None else acc + term
        out[p * PB : (p + 1) * PB, :] = acc


def exponent(peak):
    return jnp.floor(jnp.log(jnp.maximum(peak, 1e-30)) * LOG2E + 1.02)


def codes_kernel(pb, sb, days, own, other, codes, meta, mine, wide, flat, turned):
    width = own.shape[1]
    half = codes.shape[1]
    nsb = own.shape[0] // SB
    k = lax.axis_index("day")
    q = lax.axis_index("sec")
    core = k % 2
    first = (k - core) * width
    row = q * mine.shape[0]
    near = pl.ds(pl.multiple_of((row // PB) * PB, PB), PB)
    count = days.shape[1]
    one = jnp.int32(1)
    i8 = lax.broadcasted_iota(jnp.int32, (8, count), 0)
    bits = jnp.zeros((8, count), jnp.int32)
    for j in range(0, TAIL, 8):
        n = min(8, TAIL - j)
        here = days[j : j + n, :] - first
        inside = (here >= 0) & (here < 2 * width)
        word = jnp.where(inside, here & 7, 8)
        bit = lax.shift_left(jnp.full((n, count), one), jnp.where(inside, here >> 3, 0))
        for r in range(n):
            bits = bits | jnp.where(i8 == word[r : r + 1], bit[r : r + 1], 0)
    for b in range(2 * width // 8):
        wide[b * 8 : b * 8 + 8, :] = ((bits >> b) & 1).astype(jnp.float32)
    here = pl.ds(pl.multiple_of(core * width, width), width)
    there = pl.ds(pl.multiple_of((1 - core) * width, width), width)

    def rows(ref):
        parts = [ref[pl.ds(pl.multiple_of(s * SB + core * half, half), half), :] for s in range(nsb)]
        return jnp.concatenate(parts, axis=0)

    found = jnp.dot(rows(own), wide[here, :].astype(jnp.bfloat16), preferred_element_type=jnp.float32)
    found = found + jnp.dot(rows(other), wide[there, :].astype(jnp.bfloat16), preferred_element_type=jnp.float32)
    flat[...] = found
    peak = jnp.max(jnp.max(jnp.abs(found), axis=0, keepdims=True), axis=1, keepdims=True)
    power = exponent(peak)
    meta[...] = jnp.broadcast_to(power, meta.shape)
    scale = jnp.exp2(-power) * FULL
    for t in range(codes.shape[0]):
        part = flat[pl.ds(pl.multiple_of(sb[t] * half, half), half), pl.ds(pl.multiple_of(pb[t] * PB, PB), PB)]
        codes[t] = jnp.round(part * scale).astype(jnp.int32).astype(jnp.int16)
    turned[...] = wide[here, near].T
    mine[...] = turned[pl.ds(pl.multiple_of(row % PB, 8), mine.shape[0]), :]


def share_kernel(arrived, mine, codes, meta, pnl, sent):
    share = jnp.sum(arrived[...], axis=0)
    pnl[...] = share.astype(jnp.bfloat16)
    picked = jnp.sum(share * mine[...], axis=1, keepdims=True)
    shape = share.shape
    rows = lax.broadcasted_iota(jnp.int32, shape, 0)
    diag = rows == lax.broadcasted_iota(jnp.int32, shape, 1)
    line = jnp.sum(jnp.where(diag, picked, 0.0), axis=0, keepdims=True)
    power = exponent(jnp.max(jnp.abs(line), axis=1, keepdims=True))
    scaled = line * jnp.exp2(-power) * HIGH
    high = jnp.round(scaled)
    low = jnp.round((scaled - high) * FULL)
    extra = jnp.where(rows == 0, high, jnp.where(rows == 1, low, jnp.where(rows == 2, power, meta[...])))
    extra = extra.astype(jnp.int32).astype(jnp.int16)
    half = codes.shape[1]
    for k in range(sent.shape[0]):
        sent[k, :half, :] = codes[k]
        sent[k, half:, :] = extra


def tail_kernel(cnt, arrived, out, short):
    half = SB // 2
    sides = [None, None]
    total = None
    for k in range(arrived.shape[0]):
        extra = arrived[k, half:, :].astype(jnp.int32).astype(jnp.float32)
        scale = jnp.exp2(extra[3:4]) / FULL
        part = arrived[k, :half, :].astype(jnp.int32).astype(jnp.float32) * scale
        sides[k % 2] = part if sides[k % 2] is None else sides[k % 2] + part
        line = (extra[0:1] + extra[1:2] / FULL) * (jnp.exp2(extra[2:3]) / HIGH)
        total = line if total is None else total + line
    live = (lax.axis_index("day") < cnt[0]).astype(jnp.float32)
    out[0] = jnp.concatenate(sides, axis=0).T * live / TAIL
    short[...] = (-total / TAIL)[:, : short.shape[1]]


def call(kernel, outs, ins, scratch=(), limit=LIMIT, flops=10**7, moved=600000):
    several = isinstance(outs, tuple)
    return pl.pallas_call(
        kernel,
        out_shape=outs,
        in_specs=[spec(i) for i in ins],
        out_specs=tuple(spec(VMEM) for _ in outs) if several else spec(VMEM),
        scratch_shapes=list(scratch),
        cost_estimate=pl.CostEstimate(flops=flops, bytes_accessed=moved, transcendentals=0),
        compiler_params=pltpu.CompilerParams(vmem_limit_bytes=limit),
    )


def step(sec_pnl, holdings, tile_pblock, tile_sblock, tile_count, tail_days):
    n_day = lax.axis_size("day")
    n_sec = lax.axis_size("sec")
    width = sec_pnl.shape[1]
    slots = holdings.shape[0]
    portfolios = tail_days.shape[0]
    rows = portfolios // n_sec
    half = SB // 2
    f32 = jnp.float32
    shape = jax.ShapeDtypeStruct
    partial = call(
        partial_kernel,
        shape((portfolios, width), f32),
        [SMEM] * 3 + [VMEM] * 2,
        [pltpu.SMEM((slots,), jnp.int32)],
        limit=None,
    )(tile_pblock, tile_sblock, tile_count, sec_pnl, holdings)
    arrived = exchange(partial.reshape(n_sec, rows, width), "sec")
    other = lax.ppermute(sec_pnl, "day", [(i, i ^ 1) for i in range(n_day)])
    codes, meta, mine = call(
        codes_kernel,
        (shape((slots, half, PB), jnp.int16), shape((8, PB), f32), shape((rows, width), f32)),
        [SMEM] * 2 + [VMEM] * 3,
        [
            pltpu.VMEM((2 * width, portfolios), f32),
            pltpu.VMEM((sec_pnl.shape[0] // 2, portfolios), f32),
            pltpu.VMEM((PB, width), f32),
        ],
    )(tile_pblock, tile_sblock, tail_days.T, sec_pnl, other)
    pnl, sent = call(
        share_kernel, (shape((rows, width), jnp.bfloat16), shape((n_day, half + 8, PB), jnp.int16)), [VMEM] * 4
    )(arrived, mine, codes, meta)
    back = exchange(sent, "day")
    tail_mean, short = call(
        tail_kernel, (shape((1, PB, SB), f32), shape((1, rows), f32)), [SMEM, VMEM]
    )(tile_count, back)
    return pnl, short.reshape(rows), tail_mean


def solution(mesh):
    placed = (P("sec", "day"), P("sec", None, None), P("sec"), P("sec"), P("sec"), P())
    return jax.shard_map(
        step,
        mesh=mesh,
        in_specs=placed,
        out_specs=(P("sec", "day"), P("sec"), P(("sec", "day"), None, None)),
        check_vma=False,
    )
```

```python
import jax
import jax.numpy as jnp
from jax import lax
from jax.experimental import pallas as pl
from jax.experimental.pallas import tpu as pltpu
from jax.sharding import PartitionSpec as P


SB = 128
PB = 128
TAIL = 103
TEAM = 4
LIMIT = 4 * 1024 * 1024
LOG2E = 1.4426950408889634
FULL = 32000.0
HIGH = 16000.0
VMEM = pltpu.VMEM
SMEM = pltpu.SMEM


def spec(space):
    return pl.BlockSpec(memory_space=space)


def exchange(x, axis):
    return lax.all_to_all(x, axis, split_axis=0, concat_axis=0, tiled=True)


def partial_kernel(pb, sb, cnt, sec, hold, out, inv):
    slots = hold.shape[0]
    nsb = sec.shape[0] // SB
    npb = slots // nsb
    for t in range(slots):
        inv[pb[t] * nsb + sb[t]] = t
    for p in range(npb):
        acc = None
        for s in range(nsb):
            t = inv[p * nsb + s]
            live = (t < cnt[...]).astype(jnp.float32)
            term = live * jnp.dot(hold[t], sec[s * SB : (s + 1) * SB, :], preferred_element_type=jnp.float32)
            acc = term if acc is None else acc + term
        out[p * PB : (p + 1) * PB, :] = acc


def exponent(peak):
    return jnp.floor(jnp.log(jnp.maximum(peak, 1e-30)) * LOG2E + 1.02)


def pack_kernel(sec, *outs):
    part = SB // TEAM
    seat = lax.axis_index("day") % TEAM
    for j, out in enumerate(outs):
        at = (seat ^ (j + 1)) * part
        for s in range(sec.shape[0] // SB):
            out[s * part : (s + 1) * part, :] = sec[pl.ds(pl.multiple_of(s * SB + at, part), part), :]


def codes_kernel(pb, sb, days, own, *refs):
    others = refs[: TEAM - 1]
    codes, meta, mine, wide, flat, turned = refs[TEAM - 1 :]
    width = own.shape[1]
    part = codes.shape[1]
    nsb = own.shape[0] // SB
    k = lax.axis_index("day")
    q = lax.axis_index("sec")
    seat = k % TEAM
    first = (k - seat) * width
    row = q * mine.shape[0]
    near = pl.ds(pl.multiple_of((row // PB) * PB, PB), PB)
    count = days.shape[1]
    deep = TEAM * width // 32
    one = jnp.int32(1)
    at = lax.broadcasted_iota(jnp.int32, (deep, count), 0)
    bits = jnp.zeros((deep, count), jnp.int32)
    for j in range(0, TAIL, 8):
        n = min(8, TAIL - j)
        here = days[j : j + n, :] - first
        inside = (here >= 0) & (here < TEAM * width)
        word = jnp.where(inside, here & (deep - 1), deep)
        bit = lax.shift_left(jnp.full((n, count), one), jnp.where(inside, here // deep, 0))
        for r in range(n):
            bits = bits | jnp.where(at == word[r : r + 1], bit[r : r + 1], 0)
    for b in range(32):
        wide[b * deep : (b + 1) * deep, :] = ((bits >> b) & 1).astype(jnp.float32)

    def span(member):
        return pl.ds(pl.multiple_of(member * width, width), width)

    rows = [own[pl.ds(pl.multiple_of(s * SB + seat * part, part), part), :] for s in range(nsb)]
    rows = [jnp.concatenate(rows, axis=0)] + [other[...] for other in others]
    found = None
    for j in range(TEAM):
        term = jnp.dot(rows[j], wide[span(seat ^ j), :].astype(jnp.bfloat16), preferred_element_type=jnp.float32)
        found = term if found is None else found + term
    flat[...] = found
    peak = jnp.max(jnp.max(jnp.abs(found), axis=0, keepdims=True), axis=1, keepdims=True)
    power = exponent(peak)
    meta[...] = jnp.broadcast_to(power, meta.shape)
    scale = jnp.exp2(-power) * FULL
    for t in range(codes.shape[0]):
        tile = flat[pl.ds(pl.multiple_of(sb[t] * part, part), part), pl.ds(pl.multiple_of(pb[t] * PB, PB), PB)]
        codes[t] = jnp.round(tile * scale).astype(jnp.int32).astype(jnp.int16)
    turned[...] = wide[span(seat), near].T
    mine[...] = turned[pl.ds(pl.multiple_of(row % PB, 8), mine.shape[0]), :]


def share_kernel(arrived, mine, codes, meta, pnl, sent):
    share = jnp.sum(arrived[...], axis=0)
    pnl[...] = share.astype(jnp.bfloat16)
    picked = jnp.sum(share * mine[...], axis=1, keepdims=True)
    shape = share.shape
    rows = lax.broadcasted_iota(jnp.int32, shape, 0)
    diag = rows == lax.broadcasted_iota(jnp.int32, shape, 1)
    line = jnp.sum(jnp.where(diag, picked, 0.0), axis=0, keepdims=True)
    power = exponent(jnp.max(jnp.abs(line), axis=1, keepdims=True))
    scaled = line * jnp.exp2(-power) * HIGH
    high = jnp.round(scaled)
    low = jnp.round((scaled - high) * FULL)
    extra = jnp.where(rows == 0, high, jnp.where(rows == 1, low, jnp.where(rows == 2, power, meta[...])))
    extra = extra.astype(jnp.int32).astype(jnp.int16)
    part = codes.shape[1]
    for k in range(sent.shape[0]):
        sent[k, :part, :] = codes[k]
        sent[k, part:, :] = extra


def tail_kernel(cnt, arrived, out, short):
    part = SB // TEAM
    sides = [None] * TEAM
    total = None
    for k in range(arrived.shape[0]):
        extra = arrived[k, part:, :].astype(jnp.int32).astype(jnp.float32)
        scale = jnp.exp2(extra[3:4]) / FULL
        here = arrived[k, :part, :].astype(jnp.int32).astype(jnp.float32) * scale
        sides[k % TEAM] = here if sides[k % TEAM] is None else sides[k % TEAM] + here
        line = (extra[0:1] + extra[1:2] / FULL) * (jnp.exp2(extra[2:3]) / HIGH)
        total = line if total is None else total + line
    live = (lax.axis_index("day") < cnt[...]).astype(jnp.float32)
    out[0] = jnp.concatenate(sides, axis=0).T * live / TAIL
    short[...] = (-total / TAIL)[:, : short.shape[1]]


def call(kernel, outs, ins, scratch=(), limit=LIMIT, flops=10**7, moved=600000):
    several = isinstance(outs, tuple)
    return pl.pallas_call(
        kernel,
        out_shape=outs,
        in_specs=[spec(i) for i in ins],
        out_specs=tuple(spec(VMEM) for _ in outs) if several else spec(VMEM),
        scratch_shapes=list(scratch),
        cost_estimate=pl.CostEstimate(flops=flops, bytes_accessed=moved, transcendentals=0),
        compiler_params=pltpu.CompilerParams(vmem_limit_bytes=limit),
    )


def step(sec_pnl, holdings, tile_pblock, tile_sblock, tile_count, tail_days):
    n_day = lax.axis_size("day")
    n_sec = lax.axis_size("sec")
    width = sec_pnl.shape[1]
    slots = holdings.shape[0]
    portfolios = tail_days.shape[0]
    rows = portfolios // n_sec
    part = SB // TEAM
    f32 = jnp.float32
    shape = jax.ShapeDtypeStruct
    count = tile_count.reshape(1, 1)
    partial = call(
        partial_kernel,
        shape((portfolios, width), f32),
        [SMEM] * 2 + [VMEM] * 3,
        [pltpu.SMEM((slots,), jnp.int32)],
        limit=None,
    )(tile_pblock, tile_sblock, count, sec_pnl, holdings)
    arrived = exchange(partial.reshape(n_sec, rows, width), "sec")
    packs = call(
        pack_kernel, tuple(shape((sec_pnl.shape[0] // TEAM, width), sec_pnl.dtype) for _ in range(TEAM - 1)), [VMEM]
    )(sec_pnl)
    others = [None] * (TEAM - 1)
    for j in (3, 2, 1):
        others[j - 1] = lax.ppermute(packs[j - 1], "day", [(i, i ^ j) for i in range(n_day)])
    codes, meta, mine = call(
        codes_kernel,
        (shape((slots, part, PB), jnp.int16), shape((8, PB), f32), shape((rows, width), f32)),
        [SMEM] * 2 + [VMEM] * (TEAM + 1),
        [
            pltpu.VMEM((TEAM * width, portfolios), f32),
            pltpu.VMEM((sec_pnl.shape[0] // TEAM, portfolios), f32),
            pltpu.VMEM((PB, width), f32),
        ],
    )(tile_pblock, tile_sblock, tail_days.T, sec_pnl, *others)
    pnl, sent = call(
        share_kernel, (shape((rows, width), jnp.bfloat16), shape((n_day, part + 8, PB), jnp.int16)), [VMEM] * 4
    )(arrived, mine, codes, meta)
    back = exchange(sent, "day")
    tail_mean, short = call(tail_kernel, (shape((1, PB, SB), f32), shape((1, rows), f32)), [VMEM] * 2)(count, back)
    return pnl, short.reshape(rows), tail_mean


def solution(mesh):
    placed = (P("sec", "day"), P("sec", None, None), P("sec"), P("sec"), P("sec"), P())
    return jax.shard_map(
        step,
        mesh=mesh,
        in_specs=placed,
        out_specs=(P("sec", "day"), P("sec"), P(("sec", "day"), None, None)),
        check_vma=False,
    )
```

```python
import jax
import jax.numpy as jnp
from jax import lax
from jax.experimental import pallas as pl
from jax.experimental.pallas import tpu as pltpu
from jax.sharding import PartitionSpec as P


SB = 128
PB = 128
TAIL = 103
TEAM = 4
LIMIT = 4 * 1024 * 1024
LOG2E = 1.4426950408889634
FULL = 32000.0
HIGH = 16000.0
VMEM = pltpu.VMEM
SMEM = pltpu.SMEM


def spec(space):
    return pl.BlockSpec(memory_space=space)


def exchange(x, axis):
    return lax.all_to_all(x, axis, split_axis=0, concat_axis=0, tiled=True)


def partial_kernel(pb, sb, cnt, sec, hold, out, inv):
    slots = hold.shape[0]
    nsb = sec.shape[0] // SB
    npb = slots // nsb
    for t in range(slots):
        inv[pb[t] * nsb + sb[t]] = t
    for p in range(npb):
        acc = None
        for s in range(nsb):
            t = inv[p * nsb + s]
            live = (t < cnt[...]).astype(jnp.float32)
            term = live * jnp.dot(hold[t], sec[s * SB : (s + 1) * SB, :], preferred_element_type=jnp.float32)
            acc = term if acc is None else acc + term
        out[p * PB : (p + 1) * PB, :] = acc


def exponent(peak):
    return jnp.floor(jnp.log(jnp.maximum(peak, 1e-30)) * LOG2E + 1.02)


def pack_kernel(sec, *outs):
    part = SB // TEAM
    seat = lax.axis_index("day") % TEAM
    for j, out in enumerate(outs):
        at = (seat ^ (j + 1)) * part
        for s in range(sec.shape[0] // SB):
            out[s * part : (s + 1) * part, :] = sec[pl.ds(pl.multiple_of(s * SB + at, part), part), :]


def mask_kernel(pb, sb, days, own, wide, base, mine, turned):
    width = own.shape[1]
    part = SB // TEAM
    q = lax.axis_index("sec")
    k = lax.axis_index("day")
    seat = k % TEAM
    first = (k - seat) * width
    row = q * mine.shape[0]
    near = pl.ds(pl.multiple_of((row // PB) * PB, PB), PB)
    count = days.shape[1]
    deep = TEAM * width // 32
    one = jnp.int32(1)
    at = lax.broadcasted_iota(jnp.int32, (deep, count), 0)
    bits = jnp.zeros((deep, count), jnp.int32)
    for j in range(0, TAIL, 8):
        n = min(8, TAIL - j)
        here = days[j : j + n, :] - first
        inside = (here >= 0) & (here < TEAM * width)
        word = jnp.where(inside, here & (deep - 1), deep)
        bit = lax.shift_left(jnp.full((n, count), one), jnp.where(inside, here // deep, 0))
        for r in range(n):
            bits = bits | jnp.where(at == word[r : r + 1], bit[r : r + 1], 0)
    for b in range(32):
        wide[b * deep : (b + 1) * deep, :] = ((bits >> b) & 1).astype(jnp.float32).astype(jnp.bfloat16)
    span = pl.ds(pl.multiple_of(seat * width, width), width)
    rows = [own[pl.ds(pl.multiple_of(s * SB + seat * part, part), part), :] for s in range(own.shape[0] // SB)]
    base[...] = jnp.dot(jnp.concatenate(rows, axis=0), wide[span, :], preferred_element_type=jnp.float32)
    turned[...] = wide[span, near].astype(jnp.float32).T
    mine[...] = turned[pl.ds(pl.multiple_of(row % PB, 8), mine.shape[0]), :]


def codes_kernel(pb, sb, wide, base, *refs):
    others = refs[: TEAM - 1]
    codes, meta, flat = refs[TEAM - 1 :]
    part = codes.shape[1]
    width = wide.shape[0] // TEAM
    seat = lax.axis_index("day") % TEAM
    found = base[...]
    for j in range(1, TEAM):
        span = pl.ds(pl.multiple_of((seat ^ j) * width, width), width)
        found = found + jnp.dot(others[j - 1][...], wide[span, :], preferred_element_type=jnp.float32)
    flat[...] = found
    peak = jnp.max(jnp.max(jnp.abs(found), axis=0, keepdims=True), axis=1, keepdims=True)
    power = exponent(peak)
    meta[...] = jnp.broadcast_to(power, meta.shape)
    scale = jnp.exp2(-power) * FULL
    for t in range(codes.shape[0]):
        tile = flat[pl.ds(pl.multiple_of(sb[t] * part, part), part), pl.ds(pl.multiple_of(pb[t] * PB, PB), PB)]
        codes[t] = jnp.round(tile * scale).astype(jnp.int32).astype(jnp.int16)


def share_kernel(arrived, mine, codes, meta, pnl, sent):
    share = jnp.sum(arrived[...], axis=0)
    pnl[...] = share.astype(jnp.bfloat16)
    picked = jnp.sum(share * mine[...], axis=1, keepdims=True)
    shape = share.shape
    rows = lax.broadcasted_iota(jnp.int32, shape, 0)
    diag = rows == lax.broadcasted_iota(jnp.int32, shape, 1)
    line = jnp.sum(jnp.where(diag, picked, 0.0), axis=0, keepdims=True)
    power = exponent(jnp.max(jnp.abs(line), axis=1, keepdims=True))
    scaled = line * jnp.exp2(-power) * HIGH
    high = jnp.round(scaled)
    low = jnp.round((scaled - high) * FULL)
    extra = jnp.where(rows == 0, high, jnp.where(rows == 1, low, jnp.where(rows == 2, power, meta[...])))
    extra = extra.astype(jnp.int32).astype(jnp.int16)
    part = codes.shape[1]
    for k in range(sent.shape[0]):
        sent[k, :part, :] = codes[k]
        sent[k, part:, :] = extra


def tail_kernel(cnt, arrived, out, short):
    part = SB // TEAM
    sides = [None] * TEAM
    total = None
    for k in range(arrived.shape[0]):
        extra = arrived[k, part:, :].astype(jnp.int32).astype(jnp.float32)
        scale = jnp.exp2(extra[3:4]) / FULL
        here = arrived[k, :part, :].astype(jnp.int32).astype(jnp.float32) * scale
        sides[k % TEAM] = here if sides[k % TEAM] is None else sides[k % TEAM] + here
        line = (extra[0:1] + extra[1:2] / FULL) * (jnp.exp2(extra[2:3]) / HIGH)
        total = line if total is None else total + line
    live = (lax.axis_index("day") < cnt[...]).astype(jnp.float32)
    out[0] = jnp.concatenate(sides, axis=0).T * live / TAIL
    short[...] = (-total / TAIL)[:, : short.shape[1]]


def call(kernel, outs, ins, scratch=(), limit=LIMIT, flops=10**7, moved=600000):
    several = isinstance(outs, tuple)
    return pl.pallas_call(
        kernel,
        out_shape=outs,
        in_specs=[spec(i) for i in ins],
        out_specs=tuple(spec(VMEM) for _ in outs) if several else spec(VMEM),
        scratch_shapes=list(scratch),
        cost_estimate=pl.CostEstimate(flops=flops, bytes_accessed=moved, transcendentals=0),
        compiler_params=pltpu.CompilerParams(vmem_limit_bytes=limit),
    )


def step(sec_pnl, holdings, tile_pblock, tile_sblock, tile_count, tail_days):
    n_day = lax.axis_size("day")
    n_sec = lax.axis_size("sec")
    width = sec_pnl.shape[1]
    slots = holdings.shape[0]
    portfolios = tail_days.shape[0]
    rows = portfolios // n_sec
    part = SB // TEAM
    f32 = jnp.float32
    shape = jax.ShapeDtypeStruct
    count = tile_count.reshape(1, 1)
    partial = call(
        partial_kernel,
        shape((portfolios, width), f32),
        [SMEM] * 2 + [VMEM] * 3,
        [pltpu.SMEM((slots,), jnp.int32)],
        limit=None,
    )(tile_pblock, tile_sblock, count, sec_pnl, holdings)
    arrived = exchange(partial.reshape(n_sec, rows, width), "sec")
    packs = call(
        pack_kernel, tuple(shape((sec_pnl.shape[0] // TEAM, width), sec_pnl.dtype) for _ in range(TEAM - 1)), [VMEM]
    )(sec_pnl)
    others = [None] * (TEAM - 1)
    for j in (3, 2, 1):
        others[j - 1] = lax.ppermute(packs[j - 1], "day", [(i, i ^ j) for i in range(n_day)])
    group = sec_pnl.shape[0] // TEAM
    wide, base, mine = call(
        mask_kernel,
        (shape((TEAM * width, portfolios), jnp.bfloat16), shape((group, portfolios), f32), shape((rows, width), f32)),
        [SMEM] * 2 + [VMEM] * 2,
        [pltpu.VMEM((PB, width), f32)],
    )(tile_pblock, tile_sblock, tail_days.T, sec_pnl)
    codes, meta = call(
        codes_kernel,
        (shape((slots, part, PB), jnp.int16), shape((8, PB), f32)),
        [SMEM] * 2 + [VMEM] * (TEAM + 1),
        [pltpu.VMEM((group, portfolios), f32)],
    )(tile_pblock, tile_sblock, wide, base, *others)
    pnl, sent = call(
        share_kernel, (shape((rows, width), jnp.bfloat16), shape((n_day, part + 8, PB), jnp.int16)), [VMEM] * 4
    )(arrived, mine, codes, meta)
    back = exchange(sent, "day")
    tail_mean, short = call(tail_kernel, (shape((1, PB, SB), f32), shape((1, rows), f32)), [VMEM] * 2)(count, back)
    return pnl, short.reshape(rows), tail_mean


def solution(mesh):
    placed = (P("sec", "day"), P("sec", None, None), P("sec"), P("sec"), P("sec"), P())
    return jax.shard_map(
        step,
        mesh=mesh,
        in_specs=placed,
        out_specs=(P("sec", "day"), P("sec"), P(("sec", "day"), None, None)),
        check_vma=False,
    )
```

```python
import jax
import jax.numpy as jnp
from jax import lax
from jax.experimental import pallas as pl
from jax.experimental.pallas import tpu as pltpu
from jax.sharding import PartitionSpec as P


SB = 128
PB = 128
TAIL = 103
TEAM = 2
PER = 8
SEC_ROOT = 20
DAY_ROOT = 12
LIMIT = 4 * 1024 * 1024
LOG2E = 1.4426950408889634
FULL = 32000.0
HIGH = 16000.0
VMEM = pltpu.VMEM
SMEM = pltpu.SMEM


def spec(space):
    return pl.BlockSpec(memory_space=space)


def order_of(count, root):
    return [(root + i) % count for i in range(count)]


def exchange(x, axis, root):
    order = order_of(x.shape[0], root)
    return lax.all_to_all(x, axis, split_axis=0, concat_axis=0, tiled=True, axis_index_groups=[order])


def partial_kernel(pb, sb, cnt, sec, hold, out, inv):
    slots = hold.shape[0]
    nsb = sec.shape[0] // SB
    npb = slots // nsb
    for t in range(slots):
        inv[pb[t] * nsb + sb[t]] = t
    for p in range(npb):
        acc = None
        for s in range(nsb):
            t = inv[p * nsb + s]
            live = (t < cnt[...]).astype(jnp.float32)
            term = live * jnp.dot(hold[t], sec[s * SB : (s + 1) * SB, :], preferred_element_type=jnp.float32)
            acc = term if acc is None else acc + term
        for i in range(PB // PER):
            at = ((p * PB // PER + i - SEC_ROOT) % (npb * PB // PER)) * PER
            out[at : at + PER, :] = acc[i * PER : (i + 1) * PER, :]


def exponent(peak):
    return jnp.floor(jnp.log(jnp.maximum(peak, 1e-30)) * LOG2E + 1.02)


def pack_kernel(sec, *outs):
    part = SB // TEAM
    seat = lax.axis_index("day") % TEAM
    for j, out in enumerate(outs):
        at = (seat ^ (j + 1)) * part
        for s in range(sec.shape[0] // SB):
            out[s * part : (s + 1) * part, :] = sec[pl.ds(pl.multiple_of(s * SB + at, part), part), :]


def mask_kernel(pb, sb, days, own, wide, base, mine, turned):
    width = own.shape[1]
    part = SB // TEAM
    q = lax.axis_index("sec")
    k = lax.axis_index("day")
    seat = k % TEAM
    first = (k - seat) * width
    row = q * mine.shape[0]
    near = pl.ds(pl.multiple_of((row // PB) * PB, PB), PB)
    count = days.shape[1]
    deep = TEAM * width // 32
    one = jnp.int32(1)
    at = lax.broadcasted_iota(jnp.int32, (deep, count), 0)
    bits = jnp.zeros((deep, count), jnp.int32)
    for j in range(0, TAIL, 8):
        n = min(8, TAIL - j)
        here = days[j : j + n, :] - first
        inside = (here >= 0) & (here < TEAM * width)
        word = jnp.where(inside, here & (deep - 1), deep)
        bit = lax.shift_left(jnp.full((n, count), one), jnp.where(inside, here // deep, 0))
        for r in range(n):
            bits = bits | jnp.where(at == word[r : r + 1], bit[r : r + 1], 0)
    for b in range(32):
        wide[b * deep : (b + 1) * deep, :] = ((bits >> b) & 1).astype(jnp.float32).astype(jnp.bfloat16)
    span = pl.ds(pl.multiple_of(seat * width, width), width)
    rows = [own[pl.ds(pl.multiple_of(s * SB + seat * part, part), part), :] for s in range(own.shape[0] // SB)]
    base[...] = jnp.dot(jnp.concatenate(rows, axis=0), wide[span, :], preferred_element_type=jnp.float32)
    turned[...] = wide[span, near].astype(jnp.float32).T
    mine[...] = turned[pl.ds(pl.multiple_of(row % PB, 8), mine.shape[0]), :]


def share_kernel(pb, sb, arrived, mine, wide, base, *refs):
    others = refs[: TEAM - 1]
    pnl, sent, flat = refs[TEAM - 1 :]
    part = SB // TEAM
    width = wide.shape[0] // TEAM
    seat = lax.axis_index("day") % TEAM
    found = base[...]
    for j in range(1, TEAM):
        span = pl.ds(pl.multiple_of((seat ^ j) * width, width), width)
        found = found + jnp.dot(others[j - 1][...], wide[span, :], preferred_element_type=jnp.float32)
    flat[...] = found
    peak = jnp.max(jnp.max(jnp.abs(found), axis=0, keepdims=True), axis=1, keepdims=True)
    held = exponent(peak)
    scale = jnp.exp2(-held) * FULL
    for i, t in enumerate(order_of(sent.shape[0], DAY_ROOT)):
        tile = flat[pl.ds(pl.multiple_of(sb[t] * part, part), part), pl.ds(pl.multiple_of(pb[t] * PB, PB), PB)]
        sent[i, :part, :] = jnp.round(tile * scale).astype(jnp.int32).astype(jnp.int16)
    share = jnp.sum(arrived[...], axis=0)
    pnl[...] = share.astype(jnp.bfloat16)
    picked = jnp.sum(share * mine[...], axis=1, keepdims=True)
    shape = share.shape
    rows = lax.broadcasted_iota(jnp.int32, shape, 0)
    diag = rows == lax.broadcasted_iota(jnp.int32, shape, 1)
    line = jnp.sum(jnp.where(diag, picked, 0.0), axis=0, keepdims=True)
    power = exponent(jnp.max(jnp.abs(line), axis=1, keepdims=True))
    scaled = line * jnp.exp2(-power) * HIGH
    high = jnp.round(scaled)
    low = jnp.round((scaled - high) * FULL)
    extra = jnp.where(rows == 0, high, jnp.where(rows == 1, low, jnp.where(rows == 2, power, held)))
    extra = extra.astype(jnp.int32).astype(jnp.int16)
    for i in range(sent.shape[0]):
        sent[i, part:, :] = extra


def tail_kernel(cnt, arrived, out, short):
    part = SB // TEAM
    sides = [None] * TEAM
    total = None
    for i, k in enumerate(order_of(arrived.shape[0], DAY_ROOT)):
        extra = arrived[i, part:, :].astype(jnp.int32).astype(jnp.float32)
        scale = jnp.exp2(extra[3:4]) / FULL
        here = arrived[i, :part, :].astype(jnp.int32).astype(jnp.float32) * scale
        sides[k % TEAM] = here if sides[k % TEAM] is None else sides[k % TEAM] + here
        line = (extra[0:1] + extra[1:2] / FULL) * (jnp.exp2(extra[2:3]) / HIGH)
        total = line if total is None else total + line
    live = (lax.axis_index("day") < cnt[...]).astype(jnp.float32)
    out[0] = jnp.concatenate(sides, axis=0).T * live / TAIL
    short[...] = (-total / TAIL)[:, : short.shape[1]]


def call(kernel, outs, ins, scratch=(), limit=LIMIT, flops=10**7, moved=600000):
    several = isinstance(outs, tuple)
    return pl.pallas_call(
        kernel,
        out_shape=outs,
        in_specs=[spec(i) for i in ins],
        out_specs=tuple(spec(VMEM) for _ in outs) if several else spec(VMEM),
        scratch_shapes=list(scratch),
        cost_estimate=pl.CostEstimate(flops=flops, bytes_accessed=moved, transcendentals=0),
        compiler_params=pltpu.CompilerParams(vmem_limit_bytes=limit),
    )


def step(sec_pnl, holdings, tile_pblock, tile_sblock, tile_count, tail_days):
    n_day = lax.axis_size("day")
    n_sec = lax.axis_size("sec")
    width = sec_pnl.shape[1]
    slots = holdings.shape[0]
    portfolios = tail_days.shape[0]
    rows = portfolios // n_sec
    part = SB // TEAM
    f32 = jnp.float32
    shape = jax.ShapeDtypeStruct
    count = tile_count.reshape(1, 1)
    partial = call(
        partial_kernel,
        shape((portfolios, width), f32),
        [SMEM] * 2 + [VMEM] * 3,
        [pltpu.SMEM((slots,), jnp.int32)],
        limit=None,
    )(tile_pblock, tile_sblock, count, sec_pnl, holdings)
    arrived = exchange(partial.reshape(n_sec, rows, width), "sec", SEC_ROOT)
    packs = call(
        pack_kernel, tuple(shape((sec_pnl.shape[0] // TEAM, width), sec_pnl.dtype) for _ in range(TEAM - 1)), [VMEM]
    )(sec_pnl)
    others = [None] * (TEAM - 1)
    for j in range(TEAM - 1, 0, -1):
        others[j - 1] = lax.ppermute(packs[j - 1], "day", [(i, i ^ j) for i in range(n_day)])
    group = sec_pnl.shape[0] // TEAM
    wide, base, mine = call(
        mask_kernel,
        (shape((TEAM * width, portfolios), jnp.bfloat16), shape((group, portfolios), f32), shape((rows, width), f32)),
        [SMEM] * 2 + [VMEM] * 2,
        [pltpu.VMEM((PB, width), f32)],
    )(tile_pblock, tile_sblock, tail_days.T, sec_pnl)
    pnl, sent = call(
        share_kernel,
        (shape((rows, width), jnp.bfloat16), shape((n_day, part + 8, PB), jnp.int16)),
        [SMEM] * 2 + [VMEM] * (TEAM + 3),
        [pltpu.VMEM((group, portfolios), f32)],
    )(tile_pblock, tile_sblock, arrived, mine, wide, base, *others)
    back = exchange(sent, "day", DAY_ROOT)
    tail_mean, short = call(tail_kernel, (shape((1, PB, SB), f32), shape((1, rows), f32)), [VMEM] * 2)(count, back)
    return pnl, short.reshape(rows), tail_mean


def solution(mesh):
    placed = (P("sec", "day"), P("sec", None, None), P("sec"), P("sec"), P("sec"), P())
    return jax.shard_map(
        step,
        mesh=mesh,
        in_specs=placed,
        out_specs=(P("sec", "day"), P("sec"), P(("sec", "day"), None, None)),
        check_vma=False,
    )
```

```python
import jax
import jax.numpy as jnp
from jax import lax
from jax.experimental import pallas as pl
from jax.experimental.pallas import tpu as pltpu
from jax.sharding import PartitionSpec as P


SB = 128
PB = 128
TAIL = 103
TEAM = 2
PER = 8
SEC_ROOT = 28
DAY_ROOT = 12
LIMIT = 4 * 1024 * 1024
LOG2E = 1.4426950408889634
FULL = 32000.0
HIGH = 16000.0
VMEM = pltpu.VMEM
SMEM = pltpu.SMEM


def spec(space):
    return pl.BlockSpec(memory_space=space)


def order_of(count, root):
    return [(root + i) % count for i in range(count)]


def exchange(x, axis, root):
    order = order_of(x.shape[0], root)
    return lax.all_to_all(x, axis, split_axis=0, concat_axis=0, tiled=True, axis_index_groups=[order])


def partial_kernel(pb, sb, cnt, sec, hold, out, inv):
    slots = hold.shape[0]
    nsb = sec.shape[0] // SB
    npb = slots // nsb
    for t in range(slots):
        inv[pb[t] * nsb + sb[t]] = t
    for p in range(npb):
        acc = None
        for s in range(nsb):
            t = inv[p * nsb + s]
            live = (t < cnt[...]).astype(jnp.float32)
            term = live * jnp.dot(hold[t], sec[s * SB : (s + 1) * SB, :], preferred_element_type=jnp.float32)
            acc = term if acc is None else acc + term
        for i in range(PB // PER):
            at = ((p * PB // PER + i - SEC_ROOT) % (npb * PB // PER)) * PER
            out[at : at + PER, :] = acc[i * PER : (i + 1) * PER, :]


def exponent(peak):
    return jnp.floor(jnp.log(jnp.maximum(peak, 1e-30)) * LOG2E + 1.02)


def pack_kernel(sec, *outs):
    part = SB // TEAM
    seat = lax.axis_index("day") % TEAM
    for j, out in enumerate(outs):
        at = (seat ^ (j + 1)) * part
        for s in range(sec.shape[0] // SB):
            out[s * part : (s + 1) * part, :] = sec[pl.ds(pl.multiple_of(s * SB + at, part), part), :]


def mask_kernel(pb, sb, days, own, wide, base, mine, turned):
    width = own.shape[1]
    part = SB // TEAM
    q = lax.axis_index("sec")
    k = lax.axis_index("day")
    seat = k % TEAM
    first = (k - seat) * width
    row = q * mine.shape[0]
    near = pl.ds(pl.multiple_of((row // PB) * PB, PB), PB)
    count = days.shape[1]
    deep = TEAM * width // 32
    one = jnp.int32(1)
    at = lax.broadcasted_iota(jnp.int32, (deep, count), 0)
    bits = jnp.zeros((deep, count), jnp.int32)
    for j in range(0, TAIL, 8):
        n = min(8, TAIL - j)
        here = days[j : j + n, :] - first
        inside = (here >= 0) & (here < TEAM * width)
        word = jnp.where(inside, here & (deep - 1), deep)
        bit = lax.shift_left(jnp.full((n, count), one), jnp.where(inside, here // deep, 0))
        for r in range(n):
            bits = bits | jnp.where(at == word[r : r + 1], bit[r : r + 1], 0)
    for b in range(32):
        wide[b * deep : (b + 1) * deep, :] = ((bits >> b) & 1).astype(jnp.float32).astype(jnp.bfloat16)
    span = pl.ds(pl.multiple_of(seat * width, width), width)
    rows = [own[pl.ds(pl.multiple_of(s * SB + seat * part, part), part), :] for s in range(own.shape[0] // SB)]
    base[...] = jnp.dot(jnp.concatenate(rows, axis=0), wide[span, :], preferred_element_type=jnp.float32)
    turned[...] = wide[span, near].astype(jnp.float32).T
    mine[...] = turned[pl.ds(pl.multiple_of(row % PB, 8), mine.shape[0]), :]


def codes_kernel(pb, sb, wide, base, *refs):
    others = refs[: TEAM - 1]
    codes, meta, flat = refs[TEAM - 1 :]
    part = codes.shape[1]
    width = wide.shape[0] // TEAM
    seat = lax.axis_index("day") % TEAM
    found = base[...]
    for j in range(1, TEAM):
        span = pl.ds(pl.multiple_of((seat ^ j) * width, width), width)
        found = found + jnp.dot(others[j - 1][...], wide[span, :], preferred_element_type=jnp.float32)
    flat[...] = found
    peak = jnp.max(jnp.max(jnp.abs(found), axis=0, keepdims=True), axis=1, keepdims=True)
    power = exponent(peak)
    meta[...] = jnp.broadcast_to(power, meta.shape)
    scale = jnp.exp2(-power) * FULL
    for t in range(codes.shape[0]):
        tile = flat[pl.ds(pl.multiple_of(sb[t] * part, part), part), pl.ds(pl.multiple_of(pb[t] * PB, PB), PB)]
        codes[t] = jnp.round(tile * scale).astype(jnp.int32).astype(jnp.int16)


def share_kernel(arrived, mine, codes, meta, pnl, sent):
    share = jnp.sum(arrived[...], axis=0)
    pnl[...] = share.astype(jnp.bfloat16)
    picked = jnp.sum(share * mine[...], axis=1, keepdims=True)
    shape = share.shape
    rows = lax.broadcasted_iota(jnp.int32, shape, 0)
    diag = rows == lax.broadcasted_iota(jnp.int32, shape, 1)
    line = jnp.sum(jnp.where(diag, picked, 0.0), axis=0, keepdims=True)
    power = exponent(jnp.max(jnp.abs(line), axis=1, keepdims=True))
    scaled = line * jnp.exp2(-power) * HIGH
    high = jnp.round(scaled)
    low = jnp.round((scaled - high) * FULL)
    extra = jnp.where(rows == 0, high, jnp.where(rows == 1, low, jnp.where(rows == 2, power, meta[...])))
    extra = extra.astype(jnp.int32).astype(jnp.int16)
    part = codes.shape[1]
    for i, k in enumerate(order_of(sent.shape[0], DAY_ROOT)):
        sent[i, :part, :] = codes[k]
        sent[i, part:, :] = extra


def tail_kernel(cnt, arrived, out, short):
    part = SB // TEAM
    sides = [None] * TEAM
    total = None
    for i, k in enumerate(order_of(arrived.shape[0], DAY_ROOT)):
        extra = arrived[i, part:, :].astype(jnp.int32).astype(jnp.float32)
        scale = jnp.exp2(extra[3:4]) / FULL
        here = arrived[i, :part, :].astype(jnp.int32).astype(jnp.float32) * scale
        sides[k % TEAM] = here if sides[k % TEAM] is None else sides[k % TEAM] + here
        line = (extra[0:1] + extra[1:2] / FULL) * (jnp.exp2(extra[2:3]) / HIGH)
        total = line if total is None else total + line
    live = (lax.axis_index("day") < cnt[...]).astype(jnp.float32)
    out[0] = jnp.concatenate(sides, axis=0).T * live / TAIL
    short[...] = (-total / TAIL)[:, : short.shape[1]]


def call(kernel, outs, ins, scratch=(), limit=LIMIT, flops=10**7, moved=600000):
    several = isinstance(outs, tuple)
    return pl.pallas_call(
        kernel,
        out_shape=outs,
        in_specs=[spec(i) for i in ins],
        out_specs=tuple(spec(VMEM) for _ in outs) if several else spec(VMEM),
        scratch_shapes=list(scratch),
        cost_estimate=pl.CostEstimate(flops=flops, bytes_accessed=moved, transcendentals=0),
        compiler_params=pltpu.CompilerParams(vmem_limit_bytes=limit),
    )


def step(sec_pnl, holdings, tile_pblock, tile_sblock, tile_count, tail_days):
    n_day = lax.axis_size("day")
    n_sec = lax.axis_size("sec")
    width = sec_pnl.shape[1]
    slots = holdings.shape[0]
    portfolios = tail_days.shape[0]
    rows = portfolios // n_sec
    part = SB // TEAM
    f32 = jnp.float32
    shape = jax.ShapeDtypeStruct
    count = tile_count.reshape(1, 1)
    partial = call(
        partial_kernel,
        shape((portfolios, width), f32),
        [SMEM] * 2 + [VMEM] * 3,
        [pltpu.SMEM((slots,), jnp.int32)],
        limit=None,
    )(tile_pblock, tile_sblock, count, sec_pnl, holdings)
    arrived = exchange(partial.reshape(n_sec, rows, width), "sec", SEC_ROOT)
    packs = call(
        pack_kernel, tuple(shape((sec_pnl.shape[0] // TEAM, width), sec_pnl.dtype) for _ in range(TEAM - 1)), [VMEM]
    )(sec_pnl)
    others = [None] * (TEAM - 1)
    for j in range(TEAM - 1, 0, -1):
        others[j - 1] = lax.ppermute(packs[j - 1], "day", [(i, i ^ j) for i in range(n_day)])
    group = sec_pnl.shape[0] // TEAM
    wide, base, mine = call(
        mask_kernel,
        (shape((TEAM * width, portfolios), jnp.bfloat16), shape((group, portfolios), f32), shape((rows, width), f32)),
        [SMEM] * 2 + [VMEM] * 2,
        [pltpu.VMEM((PB, width), f32)],
    )(tile_pblock, tile_sblock, tail_days.T, sec_pnl)
    codes, meta = call(
        codes_kernel,
        (shape((slots, part, PB), jnp.int16), shape((8, PB), f32)),
        [SMEM] * 2 + [VMEM] * (TEAM + 1),
        [pltpu.VMEM((group, portfolios), f32)],
    )(tile_pblock, tile_sblock, wide, base, *others)
    pnl, sent = call(
        share_kernel, (shape((rows, width), jnp.bfloat16), shape((n_day, part + 8, PB), jnp.int16)), [VMEM] * 4
    )(arrived, mine, codes, meta)
    back = exchange(sent, "day", DAY_ROOT)
    tail_mean, short = call(tail_kernel, (shape((1, PB, SB), f32), shape((1, rows), f32)), [VMEM] * 2)(count, back)
    return pnl, short.reshape(rows), tail_mean


def solution(mesh):
    placed = (P("sec", "day"), P("sec", None, None), P("sec"), P("sec"), P("sec"), P())
    return jax.shard_map(
        step,
        mesh=mesh,
        in_specs=placed,
        out_specs=(P("sec", "day"), P("sec"), P(("sec", "day"), None, None)),
        check_vma=False,
    )
```
